256 devices in a mesh: rep: 4 (over x, y), ctx: 64 (over z, core).
Axes of the slice: x: 2, y: 2, z: 32, core: 2. Of those that a mesh axis runs over, the one named last changes fastest.
The devices are a block of a 4x8x32 slice.
Arguments:
- queries: bfloat16 [32768, 32, 128], P(('rep', 'ctx')), parts along dimension 0, may hold values from -128 to 128
- keys: bfloat16 [32768, 2, 128], P(('rep', 'ctx')), parts along dimension 0, may hold values from -5 to 5
- values: bfloat16 [32768, 2, 128], P(('rep', 'ctx')), parts along dimension 0, may hold values from -6 to 6
- grad_out: bfloat16 [32768, 32, 128], P(('rep', 'ctx')), parts along dimension 0, may hold values from -6 to 6
- selected: int32 [32768, 2, 8], P(('rep', 'ctx')), parts along dimension 0, may hold values from 0 to 127, as said below
Outputs:
- dquery: bfloat16 [32768, 32, 128], P(('rep', 'ctx')), parts along dimension 0
- key_grad: bfloat16 [32768, 2, 128], P(('rep', 'ctx')), parts along dimension 0
- value_grad: bfloat16 [32768, 2, 128], P(('rep', 'ctx')), parts along dimension 0
The draws below stay inside these ranges and needn't reach their ends.
There are 4 independent parts, one for each index of `rep`. The reference program is written for one: setup_inputs(seed, part) draws one part's arguments, and reference() takes and returns one part's arrays. A program takes and returns all parts, laid end to end along the dimension named above; each array names one. Nothing has to cross between parts.
Inputs may be any that keep to these rules, and one draw needn't show every extreme that they name: The 8 blocks of selected[t, g] are different and include block t // 64 and block 0. Over the 128 tokens of one device of ctx, the blocks named for one group that lie on other devices number exactly 7, at most one of each other device; block 0 is among them for every device but the first.
All inputs are finite; a program needn't handle non-finite values.
Results may differ from the reference program's by a relative error of at most 0.0075.
Values may be sent and summed in bfloat16 or wider, within the bound.
A program may use at most 128 MiB of HBM per device.

```python
import math
import jax
import jax.numpy as jnp
from jax import lax

HEADS = 32
KVG = 2
DH = 128
BLK = 64
SEL = 8
TOK_DEV = 128
BPD = 2
OTHERS = 6
FG = 7
POOLB = 9
SEQ = 8192
N_CTX = 64


def choose_blocks(key):
    base = jax.random.fold_in(key, 11)
    first, second, third, fourth = jax.random.split(base, 4)
    requesters = jnp.arange(N_CTX).astype(jnp.int32)[:, None]
    owner_ids = jnp.arange(N_CTX).astype(jnp.int32)[None, :]
    noise = jax.random.randint(first, (N_CTX, N_CTX), 0, 1 << 20)
    ranking = noise * N_CTX + owner_ids + jnp.where(owner_ids < requesters, 1 << 27, 0)
    ranking = jnp.where((owner_ids == requesters) | (owner_ids == 0), -1, ranking)
    unused, ranked = lax.top_k(ranking, FG)
    with_sink = jnp.concatenate([jnp.zeros((N_CTX, 1), jnp.int32), ranked[:, :OTHERS]], axis=1)
    owner_list = jnp.where(requesters > 0, with_sink, ranked).astype(jnp.int32)
    local_ids = jax.random.randint(second, (N_CTX, FG, KVG), 0, BPD)
    local_ids = jnp.where(owner_list[..., None] == 0, 0, local_ids)
    far_blocks = owner_list[..., None] * BPD + local_ids
    own_blocks = requesters * BPD + jnp.arange(BPD).astype(jnp.int32)[None, :]
    own_blocks = jnp.broadcast_to(own_blocks[:, :, None], (N_CTX, BPD, KVG))
    pool_ids = jnp.concatenate([own_blocks, far_blocks], axis=1).transpose(0, 2, 1)
    pool_tokens = jnp.repeat(pool_ids, TOK_DEV, axis=0)
    token_ids = jnp.arange(SEQ).astype(jnp.int32)
    slot_ids = jnp.arange(POOLB).astype(jnp.int32)
    needed = (pool_tokens == (token_ids // BLK)[:, None, None]) | (pool_tokens == 0)
    needed = needed | (slot_ids[None, None, :] == (token_ids % TOK_DEV % POOLB)[:, None, None])
    shuffle = jax.random.randint(third, (SEQ, KVG, POOLB), 0, 1 << 20)
    marks = shuffle * POOLB + slot_ids + jnp.where(needed, 1 << 26, 0)
    unused_top, picks = lax.top_k(marks, SEL)
    chosen = jnp.take_along_axis(pool_tokens, picks, axis=2)
    reorder = jax.random.randint(fourth, (SEQ, KVG, SEL), 0, 1 << 20) * SEL + jnp.arange(SEL).astype(jnp.int32)
    order = jnp.argsort(reorder, axis=2)
    return jnp.take_along_axis(chosen, order, axis=2).astype(jnp.int32)


def query_key_pair(key):
    base = jax.random.fold_in(key, 23)
    first, second = jax.random.split(base, 2)
    key_base = jnp.clip(jax.random.normal(first, (SEQ, KVG, DH), jnp.float32), -5.0, 5.0)
    key_vals = key_base
    query_vals = jnp.clip(2.0 * jax.random.normal(second, (SEQ, HEADS, DH), jnp.float32), -12.0, 12.0)
    return (query_vals, key_vals)


def draw_queries(key, part):
    query_vals, key_vals = query_key_pair(key)
    return query_vals.astype(jnp.bfloat16)


def draw_keys(key, part):
    query_vals, key_vals = query_key_pair(key)
    return key_vals.astype(jnp.bfloat16)


def draw_selected(key, part):
    return choose_blocks(key)


def block_levels(stream_key, shape, cuts, low, largest):
    level, own = 1.0, jax.random.fold_in(stream_key, 6)
    for position, blocks in cuts:
        draws = jnp.exp(jax.random.uniform(jax.random.fold_in(own, position), (blocks,), jnp.float32, low / len(cuts), largest / len(cuts)))
        level = level * jnp.repeat(draws, shape[position] // blocks).reshape([-1 if axis == position else 1 for axis in range(len(shape))])
    return level


def normal_values(stream_key, dims, deviation, reach, cuts=(), held_as=jnp.bfloat16):
    entries = jax.random.normal(stream_key, dims, jnp.float32) * deviation
    if len(cuts) > 0:
        entries = block_levels(stream_key, dims, cuts, -0.22, 0.18) * entries
    return jnp.clip(entries, min=-reach, max=reach).astype(held_as)


def setup_inputs(seed: int = 0, part: int = 0) -> dict:
    splits = jax.random.split(jax.random.key(seed), 6)
    own_keys = jax.random.split(jax.random.fold_in(splits[5], part), 6)
    return {
        "queries": draw_queries(jax.random.fold_in(jax.random.fold_in(splits[5], part), 71), part),
        "keys": draw_keys(jax.random.fold_in(jax.random.fold_in(splits[5], part), 71), part),
        "values": normal_values(own_keys[2], (SEQ, KVG, DH), 1.0, 6.0, ((0, 64),)),
        "grad_out": normal_values(own_keys[3], (SEQ, HEADS, DH), 1.0, 6.0, ((0, 64),)),
        "selected": draw_selected(jax.random.fold_in(jax.random.fold_in(splits[5], part), 71), part),
    }


def reference(queries, keys, values, grad_out, selected):
    seq_len, head_count, head_dim = queries.shape
    groups = keys.shape[1]
    per_group = head_count // groups
    scaling = 1.0 / math.sqrt(head_dim)
    tile_rows = min(seq_len, 64)
    step_count = seq_len // tile_rows
    keys_by_group = keys.transpose(1, 0, 2)
    values_by_group = values.transpose(1, 0, 2)
    group_ids = jnp.arange(groups).astype(jnp.int32)[None, :, None]
    offsets = jnp.arange(BLK).astype(jnp.int32)

    def visit(carry, inputs):
        key_acc, value_acc = carry
        query_blk, upstream, chosen, first = inputs
        positions = (chosen[..., None] * BLK + offsets).reshape(tile_rows, groups, -1).astype(jnp.int32)
        key_rows = keys_by_group[group_ids, positions].astype(jnp.float32)
        value_rows = values_by_group[group_ids, positions].astype(jnp.float32)
        query_f = query_blk.astype(jnp.float32).reshape(tile_rows, groups, per_group, head_dim)
        upstream_f = upstream.astype(jnp.float32).reshape(tile_rows, groups, per_group, head_dim)
        scores = jnp.einsum('tghd,tgld->tghl', query_f, key_rows) * scaling
        query_pos = first + jnp.arange(tile_rows).astype(jnp.int32)
        allowed = positions <= query_pos[:, None, None]
        scores = jnp.where(allowed[:, :, None, :], scores, -jnp.inf)
        row_peak = lax.optimization_barrier(jnp.max(scores, axis=-1, keepdims=True))
        weights = jnp.exp(scores - row_peak)
        weights = weights / lax.optimization_barrier(jnp.sum(weights, axis=-1, keepdims=True))
        slope_grad = jnp.einsum('tghd,tgld->tghl', upstream_f, value_rows)
        row_inner = lax.optimization_barrier(jnp.sum(weights * slope_grad, axis=-1, keepdims=True))
        dscore = lax.optimization_barrier((weights * (slope_grad - row_inner) * scaling).astype(jnp.bfloat16))
        weights_low = lax.optimization_barrier(weights.astype(jnp.bfloat16))
        dscore_f = dscore.astype(jnp.float32)
        weights_f = weights_low.astype(jnp.float32)
        dquery = jnp.einsum('tghl,tgld->tghd', dscore_f, key_rows).astype(jnp.bfloat16)
        key_part = jnp.einsum('tghl,tghd->tgld', dscore_f, query_f)
        value_part = jnp.einsum('tghl,tghd->tgld', weights_f, upstream_f)
        key_acc = key_acc.at[group_ids, positions].add(key_part)
        value_acc = value_acc.at[group_ids, positions].add(value_part)
        return ((key_acc, value_acc), dquery.reshape(tile_rows, head_count, head_dim))
    inputs = (queries.reshape(step_count, tile_rows, head_count, head_dim), grad_out.reshape(step_count, tile_rows, head_count, head_dim), selected.reshape(step_count, tile_rows, groups, -1), (jnp.arange(step_count) * tile_rows).astype(jnp.int32))
    zeros_init = jnp.zeros((groups, seq_len, head_dim), jnp.float32)
    (key_acc, value_acc), dquery = lax.scan(visit, (zeros_init, zeros_init), inputs)
    dquery = dquery.reshape(seq_len, head_count, head_dim)
    key_grad = key_acc.transpose(1, 0, 2).astype(jnp.bfloat16)
    value_grad = value_acc.transpose(1, 0, 2).astype(jnp.bfloat16)
    return (dquery, key_grad, value_grad)
```

```python
import functools
import math

import jax
import jax.numpy as jnp
from jax import lax
from jax.experimental import pallas as pl
from jax.experimental.pallas import tpu as pltpu
from jax.sharding import PartitionSpec as P

BLK = 64
CORES = 2
NEG = -1e30
MESH = pl.DeviceIdType.MESH
CHUNKS = 2


def remote(src, dst, send_sem, recv_sem, target):
    return pltpu.make_async_remote_copy(
        src_ref=src,
        dst_ref=dst,
        send_sem=send_sem,
        recv_sem=recv_sem,
        device_id={"ctx": target},
        device_id_type=MESH,
    )


def ring_ids(chips):
    me = lax.axis_index("ctx")
    chip, core = me // CORES, lax.rem(me, CORES)
    above = lax.rem(chip + 1, chips) * CORES + core
    below = lax.rem(chip + chips - 1, chips) * CORES + core
    sibling = chip * CORES + (1 - core)
    return me, chip, core, above, below, sibling


def greet(above, below, sibling):
    barrier = pltpu.get_barrier_semaphore()
    for peer in (above, below, sibling):
        pl.semaphore_signal(barrier, inc=1, device_id={"ctx": peer}, device_id_type=MESH)
    pl.semaphore_wait(barrier, 3)


def gather_kernel(
    chips, far_owner, far_local, unit_ref, table_ref, picked_ref, other_ref,
    pool, other, up_send, up_recv, dn_send, dn_recv, sib_send, sib_recv, tab_sem,
):
    me, chip, core, above, below, sibling = ring_ids(chips)
    groups = unit_ref.shape[0]
    far = far_owner.shape[1]
    n_up, n_dn = chips // 2, chips - 1 - chips // 2
    greet(above, below, sibling)

    def owner_up(step):
        return lax.rem(chip + chips - step, chips) * CORES + core

    def owner_dn(step):
        return lax.rem(chip + step, chips) * CORES + core

    def up_copy(step, part, src, owner):
        return remote(
            src, pool.at[owner, part], up_send.at[step, part], up_recv.at[step, part], above
        )

    def dn_copy(step, part, src, owner):
        return remote(
            src, pool.at[owner, part], dn_send.at[step, part], dn_recv.at[step, part], below
        )

    def sib_copy(slot, part, src, owner):
        return remote(
            src, pool.at[owner, part], sib_send.at[slot, part], sib_recv.at[slot, part], sibling
        )

    for part in range(groups):
        up_copy(0, part, unit_ref.at[part], me).start()
        dn_copy(0, part, unit_ref.at[part], me).start()
        sib_copy(0, part, unit_ref.at[part], me).start()
    tab_copy = remote(table_ref, other, tab_sem.at[0], tab_sem.at[1], sibling)
    tab_copy.start()
    pool[me] = unit_ref[...]

    def step_up(step, last):
        owner = owner_up(step)
        for part in range(groups):
            up_copy(step - 1, part, pool.at[owner, part], owner).wait_recv()
            if not last:
                up_copy(step, part, pool.at[owner, part], owner).start()
            sib_copy(step, part, pool.at[owner, part], owner).start()

    def step_dn(step, last):
        owner = owner_dn(step)
        for part in range(groups):
            dn_copy(step - 1, part, pool.at[owner, part], owner).wait_recv()
            if not last:
                dn_copy(step, part, pool.at[owner, part], owner).start()
            sib_copy(n_up + step, part, pool.at[owner, part], owner).start()

    @pl.loop(1, n_dn)
    def _(step):
        step_up(step, False)
        step_dn(step, False)

    step_up(n_dn, False)
    step_dn(n_dn, True)
    step_up(n_up, True)

    @pl.loop(0, chips)
    def _(slot):
        for part in range(groups):
            sib_copy(slot, part, unit_ref.at[part], me).wait_recv()
            sib_copy(slot, part, unit_ref.at[part], me).wait_send()

    @pl.loop(0, n_up)
    def _(step):
        for part in range(groups):
            up_copy(step, part, unit_ref.at[part], me).wait_send()

    @pl.loop(0, n_dn)
    def _(step):
        for part in range(groups):
            dn_copy(step, part, unit_ref.at[part], me).wait_send()

    tab_copy.wait()
    other_ref[...] = other[...]
    picked_ref[:, :, 0:2] = unit_ref[...]
    for group in range(groups):
        for slot in range(far):
            picked_ref[group, :, 2 + slot] = pool[
                far_owner[group, slot], group, :, far_local[group, slot]
            ]


def attend_kernel(heads, q_ref, g_ref, kv_ref, vis_ref, dq_ref, grads_ref):
    tile = pl.program_id(1)
    tokens, _, dim = q_ref.shape
    slots, blk = kv_ref.shape[2], kv_ref.shape[3]
    own = 2
    cols = tokens * heads
    scaling = 1.0 / math.sqrt(dim)
    query = q_ref[...].reshape(cols, dim)
    upstream = g_ref[...].reshape(cols, dim)
    keys = kv_ref[0, 0].reshape(slots * blk, dim)
    values = kv_ref[0, 1].reshape(slots * blk, dim)
    last = (((1,), (1,)), ((), ()))
    all_tok = vis_ref.shape[2]
    row_tok = lax.broadcasted_iota(jnp.int32, (all_tok, cols), 0)
    col_tok = lax.broadcasted_iota(jnp.int32, (all_tok, cols), 1) // heads + tile * tokens
    spread = (row_tok == col_tok).astype(jnp.bfloat16)
    seen = jnp.dot(vis_ref[0], spread, preferred_element_type=jnp.float32)
    bias = (seen - 1.0) * (-NEG)
    scores = lax.dot_general(keys, query, last, preferred_element_type=jnp.float32)
    scores = scores * (scaling * math.log2(math.e))
    key_pos = lax.broadcasted_iota(jnp.int32, (own * blk, cols), 0)
    tok_pos = lax.broadcasted_iota(jnp.int32, (own * blk, cols), 1) // heads + tile * tokens
    causal = jnp.where(key_pos <= tok_pos, 0.0, NEG)
    pieces = []
    for slot in range(slots):
        piece = scores[slot * blk : (slot + 1) * blk] + bias[slot : slot + 1]
        if slot < own:
            piece = piece + causal[slot * blk : (slot + 1) * blk]
        pieces.append(piece)
    scores = jnp.concatenate(pieces, axis=0)
    peak = jnp.max(scores, axis=0, keepdims=True)
    weights = jnp.exp2(scores - peak)
    weights = weights * (1.0 / jnp.sum(weights, axis=0, keepdims=True))
    slope = lax.dot_general(values, upstream, last, preferred_element_type=jnp.float32)
    inner = jnp.sum(weights * slope, axis=0, keepdims=True)
    dscore = (weights * (slope - inner) * scaling).astype(jnp.bfloat16)
    low = weights.astype(jnp.bfloat16)
    dquery = lax.dot_general(
        dscore, keys, (((0,), (0,)), ((), ())), preferred_element_type=jnp.float32
    )
    dq_ref[...] = dquery.astype(jnp.bfloat16).reshape(tokens, heads, dim)
    key_part = jnp.dot(dscore, query, preferred_element_type=jnp.float32)
    value_part = jnp.dot(low, upstream, preferred_element_type=jnp.float32)

    @pl.when(tile == 0)
    def _():
        grads_ref[...] = jnp.zeros_like(grads_ref)

    grads_ref[0, 0, 0:slots] += key_part.reshape(slots, blk, dim)
    grads_ref[0, 1, 0:slots] += value_part.reshape(slots, blk, dim)


def scatter_kernel(
    chips, mine, theirs, grads_ref, out_ref,
    sib, up, dn, up_send, up_recv, dn_send, dn_recv, sib_sem,
):
    me, chip, core, above, below, sibling = ring_ids(chips)
    groups = grads_ref.shape[0]
    own = 2
    n_dn, n_up = chips // 2, chips - 1 - chips // 2
    greet(above, below, sibling)
    swap = remote(grads_ref, sib, sib_sem.at[0], sib_sem.at[1], sibling)
    swap.start()
    swap.wait()

    def local_sum(owner, group, local):
        block = owner * own + local
        a = mine[group, block]
        b = theirs[group, block]
        return grads_ref[group, :, own + a] + sib[group, :, own + b]

    def dn_copy(step, part):
        return remote(
            dn.at[step, part], dn.at[step + 1, part],
            dn_send.at[step, part], dn_recv.at[step, part], below,
        )

    def up_copy(step, part):
        return remote(
            up.at[step, part], up.at[step + 1, part],
            up_send.at[step, part], up_recv.at[step, part], above,
        )

    def dn_owner(step):
        return lax.rem(chip + 2 * chips - n_dn + step, chips) * CORES + core

    def up_owner(step):
        return lax.rem(chip + n_up - step, chips) * CORES + core

    for group in range(groups):
        for buf, owner, copy in ((dn, dn_owner(0), dn_copy), (up, up_owner(0), up_copy)):
            for local in range(own):
                buf[0, group, :, local] = local_sum(owner, group, local).astype(buf.dtype)
            copy(0, group).start()

    def advance(buf, owner, copy, step):
        for group in range(groups):
            copy(step - 1, group).wait_recv()
            for local in range(own):
                total = buf[step, group, :, local].astype(jnp.float32)
                total = total + local_sum(owner, group, local)
                buf[step, group, :, local] = total.astype(buf.dtype)
            copy(step, group).start()

    @pl.loop(1, n_up)
    def _(step):
        advance(dn, dn_owner(step), dn_copy, step)
        advance(up, up_owner(step), up_copy, step)

    @pl.loop(n_up, n_dn)
    def _(step):
        advance(dn, dn_owner(step), dn_copy, step)

    for group in range(groups):
        dn_copy(n_dn - 1, group).wait_recv()
        up_copy(n_up - 1, group).wait_recv()
        for local in range(own):
            b = theirs[group, me * own + local]
            total = dn[n_dn, group, :, local].astype(jnp.float32)
            total = total + up[n_up, group, :, local].astype(jnp.float32)
            total = total + grads_ref[group, :, local] + sib[group, :, own + b]
            out_ref[group, :, local] = total.astype(out_ref.dtype)

    @pl.loop(0, n_up)
    def _(step):
        for group in range(groups):
            dn_copy(step, group).wait_send()
            up_copy(step, group).wait_send()

    @pl.loop(n_up, n_dn)
    def _(step):
        for group in range(groups):
            dn_copy(step, group).wait_send()


def local(queries, keys, values, grad_out, selected):
    tokens, head_count, dim = queries.shape
    groups = keys.shape[1]
    heads = head_count // groups
    owners = lax.axis_size("ctx")
    chips = owners // CORES
    own = tokens // BLK
    blocks = owners * own
    far = min(owners - 2, max(selected.shape[2] - own, 4)) + 1
    slots = own + far
    me = lax.axis_index("ctx")
    vmem = pl.BlockSpec(memory_space=pltpu.VMEM)
    smem = pl.BlockSpec(memory_space=pltpu.SMEM)

    unit = jnp.stack([keys, values], axis=0).transpose(2, 0, 1, 3)
    unit = unit.reshape(groups, 2, own, BLK, dim)
    sel = selected.transpose(1, 2, 0)
    block_ids = jnp.arange(blocks)
    named = jnp.any(sel[:, :, None, :] == block_ids[None, None, :, None], axis=1)
    is_far = jnp.any(named, axis=2) & (block_ids[None, :] // own != me)
    lower = (block_ids[:, None] <= block_ids[None, :]).astype(jnp.bfloat16)
    place = jnp.dot(is_far.astype(jnp.bfloat16), lower, preferred_element_type=jnp.float32)
    place = place.astype(jnp.int32) - 1
    table = jnp.where(is_far, place, far)
    picker = table[:, None, :] == jnp.arange(far)[None, :, None]
    far_block = jnp.sum(jnp.where(picker, block_ids[None, None, :], 0), axis=2)
    early = (block_ids // own < me)[None, None, :] & picker
    own_pick = block_ids[None, :] == me * own + jnp.arange(own)[:, None]
    rows = jnp.concatenate([jnp.broadcast_to(own_pick, (groups, own, blocks)), early], axis=1)
    rows = jnp.pad(rows, ((0, 0), (0, 16 - slots), (0, 0)))
    vis = jnp.einsum(
        "gsb,gbt->gst", rows.astype(jnp.bfloat16), named.astype(jnp.bfloat16),
        preferred_element_type=jnp.float32,
    ).astype(jnp.bfloat16)
    table8 = jnp.pad(table, ((0, 8 - groups), (0, 0)))

    n_half = chips // 2
    dma = pltpu.SemaphoreType.DMA
    picked, other = pl.pallas_call(
        functools.partial(gather_kernel, chips),
        out_shape=(
            jax.ShapeDtypeStruct((groups, 2, slots, BLK, dim), jnp.bfloat16),
            jax.ShapeDtypeStruct((8, blocks), jnp.int32),
        ),
        in_specs=[smem, smem, vmem, vmem],
        out_specs=(vmem, vmem),
        scratch_shapes=[
            pltpu.VMEM((owners, groups, 2, own, BLK, dim), jnp.bfloat16),
            pltpu.VMEM((8, blocks), jnp.int32),
            dma((n_half, groups)), dma((n_half, groups)),
            dma((n_half, groups)), dma((n_half, groups)),
            dma((chips, groups)), dma((chips, groups)),
            dma((2,)),
        ],
        compiler_params=pltpu.CompilerParams(collective_id=0, has_side_effects=True),
        name="gather_blocks",
    )(far_block // own, far_block % own, unit, table8)

    tile = 16
    steps = tokens // tile
    act = pl.BlockSpec((tile, heads, dim), lambda g, i: (i, g, 0))
    dquery, grads = pl.pallas_call(
        functools.partial(attend_kernel, heads),
        grid=(groups, steps),
        out_shape=(
            jax.ShapeDtypeStruct(queries.shape, jnp.bfloat16),
            jax.ShapeDtypeStruct((groups, 2, slots + 1, BLK, dim), jnp.float32),
        ),
        in_specs=[
            act, act,
            pl.BlockSpec((1, 2, slots, BLK, dim), lambda g, i: (g, 0, 0, 0, 0)),
            pl.BlockSpec((1, 16, tokens), lambda g, i: (g, 0, 0)),
        ],
        out_specs=(
            act,
            pl.BlockSpec((1, 2, slots + 1, BLK, dim), lambda g, i: (g, 0, 0, 0, 0)),
        ),
        name="attend_back",
    )(queries, grad_out, picked, vis)

    unit_shape = (groups, 2, own, BLK, dim)
    out = pl.pallas_call(
        functools.partial(scatter_kernel, chips),
        out_shape=jax.ShapeDtypeStruct(unit_shape, jnp.bfloat16),
        in_specs=[smem, smem, vmem],
        out_specs=vmem,
        scratch_shapes=[
            pltpu.VMEM((groups, 2, slots + 1, BLK, dim), jnp.float32),
            pltpu.VMEM((n_half + 1, *unit_shape), jnp.bfloat16),
            pltpu.VMEM((n_half + 1, *unit_shape), jnp.bfloat16),
            dma((n_half, groups)), dma((n_half, groups)),
            dma((n_half, groups)), dma((n_half, groups)),
            dma((2,)),
        ],
        compiler_params=pltpu.CompilerParams(collective_id=1, has_side_effects=True),
        name="scatter_sums",
    )(table, other[:groups], grads)
    both = out.transpose(1, 2, 3, 0, 4).reshape(2, tokens, groups, dim)
    return dquery, both[0], both[1]


def solution(mesh):
    spec = P(("rep", "ctx"), None, None)
    return jax.shard_map(
        local, mesh=mesh, in_specs=(spec,) * 5, out_specs=(spec,) * 3, check_vma=False
    )
```
